8 devices in a mesh: dp: 1 (over z), ep: 8 (over y, x, core).
Axes of the slice: x: 2, y: 2, z: 1, core: 2. Of those that a mesh axis runs over, the one named last changes fastest.
Arguments:
- x_in: bfloat16 [8, 16, 64, 1536], P(None, ('dp', 'ep'))
- dy_in: bfloat16 [8, 16, 64, 1536], P(None, ('dp', 'ep'))
- expert_id: int32 [8, 1, 16, 64, 8], P(None, None, ('dp', 'ep'))
- gate_vals: bfloat16 [8, 1, 16, 64, 8], P(None, None, ('dp', 'ep'))
- norm_attn: bfloat16 [1, 1536], replicated
- w_query: bfloat16 [1, 1536, 24, 64], replicated
- w_key: bfloat16 [1, 1536, 8, 64], replicated
- w_value: bfloat16 [1, 1536, 8, 64], replicated
- w_out: bfloat16 [1, 24, 64, 1536], replicated
- norm_ffn: bfloat16 [1, 1536], replicated
- s_gate: bfloat16 [1, 1536, 512], replicated
- s_up: bfloat16 [1, 1536, 512], replicated
- s_down: bfloat16 [1, 512, 1536], replicated
- e_gate: bfloat16 [1, 40, 1536, 512], P(None, 'ep')
- e_up: bfloat16 [1, 40, 1536, 512], P(None, 'ep')
- e_down: bfloat16 [1, 40, 512, 1536], P(None, 'ep')
Outputs:
- output 1: bfloat16 [8, 16, 64, 1536], P(None, ('dp', 'ep'))
- output 2: bfloat16 [8, 16, 64, 1536], P(None, ('dp', 'ep'))
- output 3: float32 [1, 1536], P('dp')
- output 4: float32 [1, 1536, 24, 64], P('dp')
- output 5: float32 [1, 1536, 8, 64], P('dp')
- output 6: float32 [1, 1536, 8, 64], P('dp')
- output 7: float32 [1, 24, 64, 1536], P('dp')
- output 8: float32 [1, 1536], P('dp')
- output 9: float32 [1, 1536, 512], P('dp')
- output 10: float32 [1, 1536, 512], P('dp')
- output 11: float32 [1, 512, 1536], P('dp')
- output 12: float32 [1, 40, 1536, 512], P('dp', 'ep')
- output 13: float32 [1, 40, 1536, 512], P('dp', 'ep')
- output 14: float32 [1, 40, 512, 1536], P('dp', 'ep')
All inputs are finite; a program needn't handle non-finite values.
Results may differ from the reference program's by a relative error of at most 0.02.
Values are sent between devices in bfloat16 or wider.
A program may use at most 1 GiB of HBM per device.

```python
import jax
import jax.numpy as jnp
from jax import lax

D = 1536
HEADS = 24
KV_HEADS = 8
HEAD = 64
EXPERTS = 40
TOP = 8
FF = 512
FS = 512
SEQS = 2
SEQ = 64
LAYERS = 1
SLOTS = 8
GROUP = 8

TOK_DEV = SEQS * SEQ
TOKENS = GROUP * TOK_DEV
ALL_SEQS = GROUP * SEQS
CAP = 8 * ((2 * TOK_DEV * TOP + 8 * EXPERTS - 1) // (8 * EXPERTS))
ROWS = GROUP * CAP
HEAD_GROUP = HEADS // KV_HEADS
EPS = 1e-6
ROPE_BASE = 10000.0


def rms_norm(values, gain_w):
    vals_f = values.astype(jnp.float32)
    inv_rms = lax.rsqrt(jnp.mean(vals_f * vals_f, axis=-1, keepdims=True) + EPS)
    return (vals_f * inv_rms * gain_w.astype(jnp.float32)).astype(jnp.bfloat16)


def rope_rotate(tensor, cos_t, sin_t):
    half_dim = HEAD // 2
    tens_f = tensor.astype(jnp.float32)
    first_half = tens_f[..., :half_dim]
    second_half = tens_f[..., half_dim:]
    return jnp.concatenate([first_half * cos_t - second_half * sin_t, second_half * cos_t + first_half * sin_t], axis=-1).astype(jnp.bfloat16)


def attend_device(blocks):
    query_heads, key_heads, value_heads = blocks
    scores = jnp.einsum('nqhgk,nshk->nhgqs', query_heads.astype(jnp.float32), key_heads.astype(jnp.float32)) * HEAD ** -0.5
    causal = jnp.arange(SEQ)[:, None] >= jnp.arange(SEQ)[None, :]
    attn_prob = jax.nn.softmax(jnp.where(causal, scores, -1e30), axis=-1).astype(jnp.bfloat16)
    return jnp.einsum('nhgqs,nshk->nqhgk', attn_prob.astype(jnp.float32), value_heads.astype(jnp.float32)).astype(jnp.bfloat16)


def attention_block(act_in, norm_a, w_query, w_key, w_value, w_out, norm_f):
    normed = rms_norm(act_in, norm_a)
    normed_f = normed.astype(jnp.float32)
    query_heads = jnp.einsum('nsd,dhk->nshk', normed_f, w_query.astype(jnp.float32)).astype(jnp.bfloat16)
    key_heads = jnp.einsum('nsd,dhk->nshk', normed_f, w_key.astype(jnp.float32)).astype(jnp.bfloat16)
    value_heads = jnp.einsum('nsd,dhk->nshk', normed_f, w_value.astype(jnp.float32)).astype(jnp.bfloat16)
    position = jnp.arange(SEQ, dtype=jnp.float32)
    inv_freq = ROPE_BASE ** (-jnp.arange(HEAD // 2, dtype=jnp.float32) / (HEAD // 2))
    angle_t = position[:, None] * inv_freq[None, :]
    cos_t = jnp.cos(angle_t)[:, None, :]
    sin_t = jnp.sin(angle_t)[:, None, :]
    query_heads = rope_rotate(query_heads, cos_t, sin_t).reshape(GROUP, SEQS, SEQ, KV_HEADS, HEAD_GROUP, HEAD)
    key_heads = rope_rotate(key_heads, cos_t, sin_t).reshape(GROUP, SEQS, SEQ, KV_HEADS, HEAD)
    value_heads = value_heads.reshape(GROUP, SEQS, SEQ, KV_HEADS, HEAD)
    mixed = lax.map(attend_device, (query_heads, key_heads, value_heads)).reshape(ALL_SEQS, SEQ, HEADS, HEAD)
    attn_out = jnp.einsum('nqhk,hkd->nqd', mixed.astype(jnp.float32), w_out.astype(jnp.float32))
    hidden = (act_in.astype(jnp.float32) + attn_out).astype(jnp.bfloat16)
    return hidden, rms_norm(hidden, norm_f)


def swiglu_shared(normed, s_gate, s_up, s_down):
    gate_act = jnp.dot(normed, s_gate, preferred_element_type=jnp.float32).astype(jnp.bfloat16)
    up_act = jnp.dot(normed, s_up, preferred_element_type=jnp.float32).astype(jnp.bfloat16)
    inner = (jax.nn.silu(gate_act.astype(jnp.float32)) * up_act.astype(jnp.float32)).astype(jnp.bfloat16)
    return jnp.dot(inner, s_down, preferred_element_type=jnp.float32)


def one_expert(blocks):
    rows_in, w_gate, w_up, w_down = blocks
    gate_act = jnp.dot(rows_in, w_gate, preferred_element_type=jnp.float32).astype(jnp.bfloat16)
    up_act = jnp.dot(rows_in, w_up, preferred_element_type=jnp.float32).astype(jnp.bfloat16)
    inner = (jax.nn.silu(gate_act.astype(jnp.float32)) * up_act.astype(jnp.float32)).astype(jnp.bfloat16)
    return jnp.dot(inner, w_down, preferred_element_type=jnp.float32).astype(jnp.bfloat16)


def expert_rows(expert_id):
    per_dev = expert_id.reshape(GROUP, TOK_DEV * TOP)
    one_hot = (per_dev[:, :, None] == jnp.arange(EXPERTS)[None, None, :]).astype(jnp.int32)
    row_rank = jnp.sum((jnp.cumsum(one_hot, axis=1) - 1) * one_hot, axis=2)
    return (jnp.arange(GROUP)[:, None] * CAP + row_rank).reshape(TOKENS, TOP)


def routed_experts(normed, expert_id, gate_vals, e_gate, e_up, e_down):
    row_pos = expert_rows(expert_id)
    buffer = jnp.zeros((EXPERTS, ROWS, D), jnp.bfloat16).at[expert_id, row_pos].set(normed[:, None, :])
    outputs = lax.map(one_expert, (buffer, e_gate, e_up, e_down))
    routed_sum = jnp.zeros((TOKENS, D), jnp.float32)
    for choice in range(TOP):
        picked = outputs[expert_id[:, choice], row_pos[:, choice]]
        routed_sum = routed_sum + gate_vals[:, choice:choice + 1].astype(jnp.float32) * picked.astype(jnp.float32)
    return routed_sum


def block_forward(act_in, dense_l, expert_l, route_l):
    norm_a, w_query, w_key, w_value, w_out, norm_f, s_gate, s_up, s_down = dense_l
    e_gate, e_up, e_down = expert_l
    expert_id, gate_vals = route_l
    hidden, normed = attention_block(act_in, norm_a, w_query, w_key, w_value, w_out, norm_f)
    normed_flat = normed.reshape(TOKENS, D)
    shared = swiglu_shared(normed_flat, s_gate, s_up, s_down)
    routed = routed_experts(normed_flat, expert_id, gate_vals, e_gate, e_up, e_down)
    out_flat = hidden.reshape(TOKENS, D).astype(jnp.float32) + shared + routed
    return out_flat.astype(jnp.bfloat16).reshape(ALL_SEQS, SEQ, D)


def stack_forward(act_in, dense, experts, routing):
    def layer_step(carry, layer_in):
        dense_l, expert_l, route_l = layer_in
        return block_forward(carry, dense_l, expert_l, route_l), None
    final_act, layer_outs = lax.scan(layer_step, act_in, (dense, experts, routing))
    return final_act


def draw_scaled(key, shape, scale):
    return (jax.random.normal(key, shape, jnp.float32) * scale).astype(jnp.bfloat16)


def draw_gain(key, shape):
    return (1.0 + 0.2 * jax.random.normal(key, shape, jnp.float32)).astype(jnp.bfloat16)


def route_device(key):
    key_perm, key_hot, key_mix = jax.random.split(key, 3)
    cells = EXPERTS * CAP
    score = jax.random.permutation(key_perm, cells)
    hot_expert = jax.random.randint(key_hot, (), 0, EXPERTS)
    score = jnp.where(jnp.arange(cells) // CAP == hot_expert, score - cells, score)
    chosen = jnp.argsort(score)[:TOK_DEV * TOP]
    chosen = chosen[jax.random.permutation(key_mix, TOK_DEV * TOP)]
    return (chosen // CAP).astype(jnp.int32).reshape(TOK_DEV, TOP)


def setup_inputs(seed: int = 0, part: int = 0) -> dict:
    weight_keys = jax.random.split(jax.random.key(seed), 12)
    part_key = jax.random.fold_in(jax.random.key(seed + 1), part)
    key_x, key_dy, key_gate, key_route = jax.random.split(part_key, 4)
    route_keys = jax.random.split(key_route, SLOTS * LAYERS * GROUP)
    expert_id = jax.vmap(route_device)(route_keys).reshape(SLOTS, LAYERS, ALL_SEQS, SEQ, TOP)
    gate_vals = (jax.random.uniform(key_gate, (SLOTS, LAYERS, ALL_SEQS, SEQ, TOP), jnp.float32, 0.5, 1.5) * TOP ** -0.5).astype(jnp.bfloat16)
    return {
        'x_in': draw_scaled(key_x, (SLOTS, ALL_SEQS, SEQ, D), 1.0),
        'dy_in': draw_scaled(key_dy, (SLOTS, ALL_SEQS, SEQ, D), 1.0),
        'expert_id': expert_id,
        'gate_vals': gate_vals,
        'norm_attn': draw_gain(weight_keys[0], (LAYERS, D)),
        'w_query': draw_scaled(weight_keys[1], (LAYERS, D, HEADS, HEAD), D ** -0.5),
        'w_key': draw_scaled(weight_keys[2], (LAYERS, D, KV_HEADS, HEAD), D ** -0.5),
        'w_value': draw_scaled(weight_keys[3], (LAYERS, D, KV_HEADS, HEAD), D ** -0.5),
        'w_out': draw_scaled(weight_keys[4], (LAYERS, HEADS, HEAD, D), 2.0 * (HEADS * HEAD) ** -0.5),
        'norm_ffn': draw_gain(weight_keys[5], (LAYERS, D)),
        's_gate': draw_scaled(weight_keys[6], (LAYERS, D, FS), D ** -0.5),
        's_up': draw_scaled(weight_keys[7], (LAYERS, D, FS), D ** -0.5),
        's_down': draw_scaled(weight_keys[8], (LAYERS, FS, D), FS ** -0.5),
        'e_gate': draw_scaled(weight_keys[9], (LAYERS, EXPERTS, D, FF), D ** -0.5),
        'e_up': draw_scaled(weight_keys[10], (LAYERS, EXPERTS, D, FF), D ** -0.5),
        'e_down': draw_scaled(weight_keys[11], (LAYERS, EXPERTS, FF, D), FF ** -0.5),
    }


def reference(x_in, dy_in, expert_id, gate_vals, norm_attn, w_query, w_key, w_value, w_out, norm_ffn, s_gate, s_up, s_down, e_gate, e_up, e_down):
    dense = (norm_attn, w_query, w_key, w_value, w_out, norm_ffn, s_gate, s_up, s_down)
    experts = (e_gate, e_up, e_down)
    ids_all = expert_id.reshape(SLOTS, LAYERS, TOKENS, TOP)
    gates_all = gate_vals.reshape(SLOTS, LAYERS, TOKENS, TOP)

    def slot_step(grad_sum, slot_in):
        x_slot, dy_slot, ids_slot, gates_slot = slot_in

        def window_fn(act_in, dense_w, expert_w):
            return stack_forward(act_in, dense_w, expert_w, (ids_slot, gates_slot))

        y_slot, pullback = jax.vjp(window_fn, x_slot, dense, experts)
        dx_slot, d_dense, d_expert = pullback(dy_slot)
        grad_sum = jax.tree.map(lambda acc_g, new_g: acc_g + new_g.astype(jnp.float32), grad_sum, (d_dense, d_expert))
        return grad_sum, (y_slot, dx_slot)

    zero_sum = jax.tree.map(lambda weight: jnp.zeros(weight.shape, jnp.float32), (dense, experts))
    grad_sum, slot_outs = lax.scan(slot_step, zero_sum, (x_in, dy_in, ids_all, gates_all))
    y_out, dx_out = slot_outs
    d_dense, d_expert = grad_sum
    return (y_out, dx_out, d_dense[0], d_dense[1], d_dense[2], d_dense[3], d_dense[4], d_dense[5], d_dense[6], d_dense[7], d_dense[8], d_expert[0], d_expert[1], d_expert[2])
```

```python
import functools

import jax
import jax.numpy as jnp
from jax import lax
from jax.experimental import pallas as pl
from jax.experimental.pallas import tpu as pltpu
from jax.sharding import PartitionSpec as P

EPS = 1e-6
ROPE_BASE = 10000.0
CAP_FACTOR = 2
F32 = jnp.float32
BF16 = jnp.bfloat16
KEY_STRIDE = 128
VMEM_BIG = 66_000_000


def capacity_of(tokens, top_k, n_exp):
    return 8 * ((CAP_FACTOR * tokens * top_k + 8 * n_exp - 1) // (8 * n_exp))


def dot_nn(lhs, rhs):
    return lax.dot_general(lhs, rhs, (((1,), (0,)), ((), ())), preferred_element_type=F32)


def dot_nt(lhs, rhs):
    return lax.dot_general(lhs, rhs, (((1,), (1,)), ((), ())), preferred_element_type=F32)


def dot_tn(lhs, rhs):
    return lax.dot_general(lhs, rhs, (((0,), (0,)), ((), ())), preferred_element_type=F32)


def rms_norm(values, gain_w):
    vals_f = values.astype(F32)
    inv_rms = lax.rsqrt(jnp.mean(vals_f * vals_f, axis=-1, keepdims=True) + EPS)
    return (vals_f * inv_rms * gain_w.astype(F32)).astype(BF16)


def rms_norm_grad(values, gain_w, d_out):
    vals_f = values.astype(F32)
    inv_rms = lax.rsqrt(jnp.mean(vals_f * vals_f, axis=-1, keepdims=True) + EPS)
    unit = vals_f * inv_rms
    d_f = d_out.astype(F32)
    d_gain = jnp.sum(d_f * unit, axis=0)
    d_unit = d_f * gain_w.astype(F32)
    d_vals = inv_rms * (d_unit - unit * jnp.mean(d_unit * unit, axis=-1, keepdims=True))
    return d_vals.astype(BF16), d_gain


def rope_rotate(tensor, cos_t, sin_t):
    half_dim = tensor.shape[-1] // 2
    tens_f = tensor.astype(F32)
    first_half = tens_f[..., :half_dim]
    second_half = tens_f[..., half_dim:]
    return jnp.concatenate([first_half * cos_t - second_half * sin_t, second_half * cos_t + first_half * sin_t], axis=-1).astype(BF16)


def attend(query, key, value, seq_len, head_dim):
    tokens = query.shape[0]
    n_seq = tokens // seq_len
    kv_heads = key.shape[1] // head_dim
    q_group = query.shape[1] // key.shape[1]
    position = jnp.arange(seq_len, dtype=F32)
    inv_freq = ROPE_BASE ** (-jnp.arange(head_dim // 2, dtype=F32) / (head_dim // 2))
    angle_t = position[:, None] * inv_freq[None, :]
    cos_t = jnp.cos(angle_t)[:, None, :]
    sin_t = jnp.sin(angle_t)[:, None, :]
    query_heads = rope_rotate(query.reshape(n_seq, seq_len, kv_heads * q_group, head_dim), cos_t, sin_t)
    query_heads = query_heads.reshape(n_seq, seq_len, kv_heads, q_group, head_dim)
    key_heads = rope_rotate(key.reshape(n_seq, seq_len, kv_heads, head_dim), cos_t, sin_t)
    value_heads = value.reshape(n_seq, seq_len, kv_heads, head_dim)
    scores = jnp.einsum('nqhgk,nshk->nhgqs', query_heads, key_heads, preferred_element_type=F32) * head_dim ** -0.5
    causal = jnp.arange(seq_len)[:, None] >= jnp.arange(seq_len)[None, :]
    attn_prob = jax.nn.softmax(jnp.where(causal, scores, -1e30), axis=-1).astype(BF16)
    mixed = jnp.einsum('nhgqs,nshk->nqhgk', attn_prob, value_heads, preferred_element_type=F32).astype(BF16)
    return mixed.reshape(tokens, kv_heads * q_group * head_dim)


def choice_keys(choice_ids, n_exp):
    n_slots, top_k, tokens = choice_ids.shape
    same = choice_ids[:, None, :, :] == jnp.arange(n_exp)[None, :, None, None]
    count = jnp.sum(same, axis=2, dtype=F32)
    before = (jnp.arange(tokens)[:, None] < jnp.arange(tokens)[None, :]).astype(BF16)
    prefix = jnp.einsum('set,tu->seu', count.astype(BF16), before, preferred_element_type=F32)
    rank = jnp.sum(jnp.where(same, prefix[:, :, None, :], 0.0), axis=1)
    earlier = jnp.arange(top_k)[:, None] > jnp.arange(top_k)[None, :]
    repeat = (choice_ids[:, :, None, :] == choice_ids[:, None, :, :]) & earlier[None, :, :, None]
    rank = rank + jnp.sum(repeat, axis=2, dtype=F32)
    return choice_ids.astype(F32) * KEY_STRIDE + rank


def expert_kernel(n_pairs, local_e, cap, key_ref, gate_ref, u_ref, dy_ref, wg_ref, wu_ref, wd_ref,
                  y_ref, du_ref, rows_ref, drows_ref, dgate_ref, dup_ref, inner_ref,
                  pick, pick_g, buf_u, buf_d):
    step = pl.program_id(1)
    tokens = u_ref.shape[1]
    d_model = u_ref.shape[2]
    top_k = key_ref.shape[2]
    pair_rows = 2 * cap

    @pl.when(step < n_pairs)
    def _gather():
        pair = step
        for exp in range(local_e):
            for src in range(2):
                row = lax.broadcasted_iota(jnp.int32, (pair_rows, tokens), 0).astype(F32) + (exp * KEY_STRIDE - src * cap)
                chosen = jnp.zeros((pair_rows, tokens), F32)
                weight = jnp.zeros((pair_rows, tokens), F32)
                for choice in range(top_k):
                    hit = key_ref[src, 0, choice:choice + 1, :] == row
                    chosen = jnp.where(hit, 1.0, chosen)
                    weight = jnp.where(hit, gate_ref[src, 0, choice:choice + 1, :], weight)
                pick[pair, pl.ds(exp * pair_rows, pair_rows), src * tokens:(src + 1) * tokens] = chosen.astype(BF16)
                pick_g[pair, pl.ds(exp * pair_rows, pair_rows), src * tokens:(src + 1) * tokens] = weight.astype(BF16)
        u_all = u_ref[...].reshape(2 * tokens, d_model)
        dy_all = dy_ref[...].reshape(2 * tokens, d_model)
        buf_u[pair] = dot_nn(pick[pair], u_all).astype(BF16)
        buf_d[pair] = dot_nn(pick_g[pair], dy_all).astype(BF16)

    @pl.when((step >= n_pairs) & (step < n_pairs + local_e))
    def _experts():
        exp = step - n_pairs
        start = pl.multiple_of(exp * pair_rows, 16)
        rows = buf_u[:, pl.ds(start, pair_rows), :].reshape(n_pairs * pair_rows, d_model)
        d_out = buf_d[:, pl.ds(start, pair_rows), :].reshape(n_pairs * pair_rows, d_model)
        rows_ref[0, 0] = rows
        drows_ref[0, 0] = d_out
        gate_f = dot_nn(rows, wg_ref[0]).astype(BF16).astype(F32)
        up_f = dot_nn(rows, wu_ref[0]).astype(BF16).astype(F32)
        sig_gate = jax.nn.sigmoid(gate_f)
        silu_gate = gate_f * sig_gate
        inner = (silu_gate * up_f).astype(BF16)
        inner_ref[0, 0] = inner
        d_inner = dot_nt(d_out, wd_ref[0]).astype(BF16).astype(F32)
        d_gate = (d_inner * up_f * sig_gate * (1.0 + gate_f * (1.0 - sig_gate))).astype(BF16)
        d_up = (d_inner * silu_gate).astype(BF16)
        dgate_ref[0, 0] = d_gate
        dup_ref[0, 0] = d_up
        result = dot_nn(inner, wd_ref[0]).astype(BF16)
        buf_u[:, pl.ds(start, pair_rows), :] = result.reshape(n_pairs, pair_rows, d_model)
        from_gate = dot_nt(d_gate, wg_ref[0]).astype(BF16).astype(F32)
        from_up = dot_nt(d_up, wu_ref[0]).astype(BF16).astype(F32)
        d_rows = (from_gate + from_up).astype(BF16)
        buf_d[:, pl.ds(start, pair_rows), :] = d_rows.reshape(n_pairs, pair_rows, d_model)

    @pl.when(step >= n_pairs + local_e)
    def _combine():
        pair = step - (n_pairs + local_e)
        y_ref[...] = dot_tn(pick_g[pair], buf_u[pair]).reshape(2, tokens, d_model)
        du_ref[...] = dot_tn(pick[pair], buf_d[pair]).reshape(2, tokens, d_model)


def expert_pass(keys, gates, u_all, dy_all, e_gate, e_up, e_down, cap, tokens):
    n_dev, n_slots, top_k, _ = keys.shape
    local_e, d_model, d_ff = e_gate.shape
    n_pairs = n_dev // 2
    exp_rows = n_dev * cap
    all_rows = n_pairs * local_e * 2 * cap
    last = n_pairs + local_e

    def pair_in(slot, step):
        return jnp.minimum(step, n_pairs - 1)

    def expert_of(slot, step):
        return jnp.clip(step - n_pairs, 0, local_e - 1)

    def pair_out(slot, step):
        return jnp.maximum(step - last, 0)

    route_spec = pl.BlockSpec((2, 1, top_k, tokens), lambda slot, step: (pair_in(slot, step), slot, 0, 0))
    token_in = pl.BlockSpec((2, tokens, d_model), lambda slot, step: (pair_in(slot, step), slot, 0))
    token_out = pl.BlockSpec((2, tokens, d_model), lambda slot, step: (pair_out(slot, step), slot, 0))
    wide = pl.BlockSpec((1, d_model, d_ff), lambda slot, step: (expert_of(slot, step), 0, 0))
    tall = pl.BlockSpec((1, d_ff, d_model), lambda slot, step: (expert_of(slot, step), 0, 0))
    save_d = pl.BlockSpec((1, 1, exp_rows, d_model), lambda slot, step: (slot, expert_of(slot, step), 0, 0))
    save_f = pl.BlockSpec((1, 1, exp_rows, d_ff), lambda slot, step: (slot, expert_of(slot, step), 0, 0))
    token_sum = jax.ShapeDtypeStruct((n_dev, n_slots * tokens, d_model), F32)
    saved_d = jax.ShapeDtypeStruct((n_slots, local_e, exp_rows, d_model), BF16)
    saved_f = jax.ShapeDtypeStruct((n_slots, local_e, exp_rows, d_ff), BF16)
    flops = n_slots * all_rows * (12 * d_model * d_ff + 8 * 2 * tokens * d_model)
    return pl.pallas_call(
        functools.partial(expert_kernel, n_pairs, local_e, cap),
        grid=(n_slots, last + n_pairs),
        in_specs=[route_spec, route_spec, token_in, token_in, wide, wide, tall],
        out_specs=[token_out, token_out, save_d, save_d, save_f, save_f, save_f],
        out_shape=[token_sum, token_sum, saved_d, saved_d, saved_f, saved_f, saved_f],
        scratch_shapes=[
            pltpu.VMEM((n_pairs, local_e * 2 * cap, 2 * tokens), BF16),
            pltpu.VMEM((n_pairs, local_e * 2 * cap, 2 * tokens), BF16),
            pltpu.VMEM((n_pairs, local_e * 2 * cap, d_model), BF16),
            pltpu.VMEM((n_pairs, local_e * 2 * cap, d_model), BF16),
        ],
        compiler_params=pltpu.CompilerParams(vmem_limit_bytes=VMEM_BIG, dimension_semantics=('arbitrary', 'arbitrary')),
        cost_estimate=pl.CostEstimate(flops=flops, bytes_accessed=n_slots * 60_000_000, transcendentals=0),
        name='expert_pass',
    )(keys, gates, u_all, dy_all, e_gate, e_up, e_down)


def expert_grad_kernel(rows_ref, drows_ref, dgate_ref, dup_ref, inner_ref, g_gate_ref, g_up_ref, g_down_ref):
    part = pl.program_id(1)
    n_slots, _, n_rows, d_model = rows_ref.shape
    d_ff = dgate_ref.shape[3]
    rows = rows_ref[...].reshape(n_slots * n_rows, d_model)
    d_out = drows_ref[...].reshape(n_slots * n_rows, d_model)
    d_gate = dgate_ref[...].reshape(n_slots * n_rows, d_ff)
    d_up = dup_ref[...].reshape(n_slots * n_rows, d_ff)
    inner = inner_ref[...].reshape(n_slots * n_rows, d_ff)

    @pl.when(part == 0)
    def _first():
        g_gate_ref[0] = dot_tn(rows, d_gate)
        g_up_ref[0] = dot_tn(rows, d_up)
        g_down_ref[0] = dot_tn(inner, d_out)

    @pl.when(part > 0)
    def _rest():
        g_gate_ref[0] += dot_tn(rows, d_gate)
        g_up_ref[0] += dot_tn(rows, d_up)
        g_down_ref[0] += dot_tn(inner, d_out)


def expert_grads(rows, d_rows, d_gate, d_up, inner, per_step):
    n_slots, local_e, n_rows, d_model = rows.shape
    d_ff = d_gate.shape[3]
    parts = n_slots // per_step
    in_d = pl.BlockSpec((per_step, 1, n_rows, d_model), lambda exp, part: (part, exp, 0, 0))
    in_f = pl.BlockSpec((per_step, 1, n_rows, d_ff), lambda exp, part: (part, exp, 0, 0))
    wide = pl.BlockSpec((1, d_model, d_ff), lambda exp, part: (exp, 0, 0))
    tall = pl.BlockSpec((1, d_ff, d_model), lambda exp, part: (exp, 0, 0))
    flops = 6 * n_slots * local_e * n_rows * d_model * d_ff
    return pl.pallas_call(
        expert_grad_kernel,
        grid=(local_e, parts),
        in_specs=[in_d, in_d, in_f, in_f, in_f],
        out_specs=[wide, wide, tall],
        out_shape=[jax.ShapeDtypeStruct((local_e, d_model, d_ff), F32)] * 2 + [jax.ShapeDtypeStruct((local_e, d_ff, d_model), F32)],
        compiler_params=pltpu.CompilerParams(vmem_limit_bytes=VMEM_BIG, dimension_semantics=('arbitrary', 'arbitrary')),
        cost_estimate=pl.CostEstimate(flops=flops, bytes_accessed=250_000_000, transcendentals=0),
        name='expert_grads',
    )(rows, d_rows, d_gate, d_up, inner)


def solution(mesh):
    n_ep = mesh.shape['ep']

    def device_fn(x_in, dy_in, expert_id, gate_vals, norm_attn, w_query, w_key, w_value, w_out, norm_ffn, s_gate, s_up, s_down, e_gate, e_up, e_down):
        n_slots, n_seq, seq_len, d_model = x_in.shape
        heads, head_dim = w_query.shape[2:]
        kv_heads = w_key.shape[2]
        top_k = expert_id.shape[-1]
        local_e = e_gate.shape[1]
        n_exp = local_e * n_ep
        tokens = n_seq * seq_len
        cap = capacity_of(tokens, top_k, n_exp)
        all_tok = n_slots * tokens
        x = x_in.reshape(all_tok, d_model)
        dy = dy_in.reshape(all_tok, d_model)
        norm_a, norm_f = norm_attn[0], norm_ffn[0]
        q_dim, kv_dim = heads * head_dim, kv_heads * head_dim
        wt_q = jnp.transpose(w_query[0], (1, 2, 0)).reshape(q_dim, d_model)
        wt_k = jnp.transpose(w_key[0], (1, 2, 0)).reshape(kv_dim, d_model)
        wt_v = jnp.transpose(w_value[0], (1, 2, 0)).reshape(kv_dim, d_model)
        wo = w_out[0].reshape(q_dim, d_model)

        ids = jnp.transpose(expert_id[:, 0], (0, 3, 1, 2)).reshape(n_slots, top_k, tokens)
        gates = jnp.transpose(gate_vals[:, 0], (0, 3, 1, 2)).reshape(n_slots, top_k, tokens).astype(F32)
        table = jnp.stack([choice_keys(ids, n_exp), gates])
        table = lax.all_gather(table, 'ep', axis=0, tiled=False)
        first_key = (lax.axis_index('ep') * (local_e * KEY_STRIDE)).astype(F32)
        keys_all = table[:, 0] - first_key
        gates_all = table[:, 1]

        dy_all = lax.all_gather(dy, 'ep', axis=0, tiled=False)

        normed = rms_norm(x, norm_a)
        query = dot_nt(normed, wt_q).astype(BF16)
        key = dot_nt(normed, wt_k).astype(BF16)
        value = dot_nt(normed, wt_v).astype(BF16)
        mixed, attend_pull = jax.vjp(functools.partial(attend, seq_len=seq_len, head_dim=head_dim), query, key, value)
        hidden = (x.astype(F32) + dot_nn(mixed, wo)).astype(BF16)
        u = rms_norm(hidden, norm_f)
        u_all = lax.all_gather(u, 'ep', axis=0, tiled=False)

        y_part, du_part, rows, d_rows, x_dgate, x_dup, x_inner = expert_pass(
            keys_all, gates_all, u_all, dy_all, e_gate[0], e_up[0], e_down[0], cap, tokens)
        routed = lax.psum_scatter(y_part, 'ep', scatter_dimension=0, tiled=False)
        d_routed = lax.psum_scatter(du_part, 'ep', scatter_dimension=0, tiled=False).astype(BF16)
        g_e_gate, g_e_up, g_e_down = expert_grads(rows, d_rows, x_dgate, x_dup, x_inner, 2)

        gate_f = dot_nn(u, s_gate[0]).astype(BF16).astype(F32)
        up_f = dot_nn(u, s_up[0]).astype(BF16).astype(F32)
        sig_gate = jax.nn.sigmoid(gate_f)
        silu_gate = gate_f * sig_gate
        inner = (silu_gate * up_f).astype(BF16)
        shared = dot_nn(inner, s_down[0])
        y = (hidden.astype(F32) + shared + routed).astype(BF16)
        d_inner = dot_nt(dy, s_down[0]).astype(BF16).astype(F32)
        d_gate = (d_inner * up_f * sig_gate * (1.0 + gate_f * (1.0 - sig_gate))).astype(BF16)
        d_up = (d_inner * silu_gate).astype(BF16)
        d_shared = dot_nt(d_gate, s_gate[0]).astype(BF16).astype(F32) + dot_nt(d_up, s_up[0]).astype(BF16).astype(F32)
        g_s_gate = dot_tn(u, d_gate)
        g_s_up = dot_tn(u, d_up)
        g_s_down = dot_tn(inner, dy)

        d_u = (d_routed.astype(F32) + d_shared.astype(BF16).astype(F32)).astype(BF16)
        d_hidden_u, g_norm_f = rms_norm_grad(hidden, norm_f, d_u)
        d_hidden = (dy.astype(F32) + d_hidden_u.astype(F32)).astype(BF16)
        d_mixed = dot_nt(d_hidden, wo).astype(BF16)
        g_out = dot_tn(mixed, d_hidden)
        d_query, d_key, d_value = attend_pull(d_mixed)
        g_q = dot_tn(d_query, normed)
        g_k = dot_tn(d_key, normed)
        g_v = dot_tn(d_value, normed)
        d_normed = (dot_nn(d_query, wt_q) + dot_nn(d_key, wt_k) + dot_nn(d_value, wt_v)).astype(BF16)
        d_x_norm, g_norm_a = rms_norm_grad(x, norm_a, d_normed)
        dx = (d_hidden.astype(F32) + d_x_norm.astype(F32)).astype(BF16)

        grads = lax.psum([g_q, g_k, g_v, g_out, g_s_gate, g_s_up, g_s_down, g_norm_a, g_norm_f], 'ep')
        g_q, g_k, g_v, g_out, g_s_gate, g_s_up, g_s_down, g_norm_a, g_norm_f = grads
        return (
            y.reshape(x_in.shape), dx.reshape(x_in.shape), g_norm_a[None],
            jnp.transpose(g_q.reshape(heads, head_dim, d_model), (2, 0, 1))[None],
            jnp.transpose(g_k.reshape(kv_heads, head_dim, d_model), (2, 0, 1))[None],
            jnp.transpose(g_v.reshape(kv_heads, head_dim, d_model), (2, 0, 1))[None],
            g_out.reshape(heads, head_dim, d_model)[None], g_norm_f[None], g_s_gate[None], g_s_up[None], g_s_down[None],
            g_e_gate[None], g_e_up[None], g_e_down[None],
        )

    tok_spec = P(None, ('dp', 'ep'), None, None)
    route_spec = P(None, None, ('dp', 'ep'), None, None)
    rep_spec = P()
    exp_spec = P(None, 'ep', None, None)
    vec_grad = P('dp', None)
    mat_grad = P('dp', None, None)
    head_grad = P('dp', None, None, None)
    exp_grad = P('dp', 'ep', None, None)
    in_specs = (tok_spec, tok_spec, route_spec, route_spec) + (rep_spec,) * 9 + (exp_spec,) * 3
    out_specs = (tok_spec, tok_spec, vec_grad, head_grad, head_grad, head_grad, head_grad, vec_grad, mat_grad, mat_grad, mat_grad, exp_grad, exp_grad, exp_grad)
    return jax.shard_map(device_fn, mesh=mesh, in_specs=in_specs, out_specs=out_specs, check_vma=False)
```

```python
import functools

import jax
import jax.numpy as jnp
from jax import lax
from jax.experimental import pallas as pl
from jax.experimental.pallas import tpu as pltpu
from jax.sharding import PartitionSpec as P


ZERO, ONE = range(2)
EPS = 1e-6
ROPE_BASE = 10000.0
CAP_FACTOR = 2
F32 = jnp.float32
BF16 = jnp.bfloat16
KEY_STRIDE = 128
VMEM_BIG = 66_000_000
CHUNKS = 4
DY_PARTS = (1, 1, 2)
U_PARTS = (1, 1, 2)
N_DEV = 8
GRAD_PARTS = ((0, 1), (1, 2), (3, 2))


def capacity_of(tokens, top_k, n_exp):
    return 8 * ((CAP_FACTOR * tokens * top_k + 8 * n_exp - 1) // (8 * n_exp))


def dot_nn(lhs, rhs):
    return lax.dot_general(lhs, rhs, (((1,), (0,)), ((), ())), preferred_element_type=F32)


def dot_nt(lhs, rhs):
    return lax.dot_general(lhs, rhs, (((1,), (1,)), ((), ())), preferred_element_type=F32)


def dot_tn(lhs, rhs):
    return lax.dot_general(lhs, rhs, (((0,), (0,)), ((), ())), preferred_element_type=F32)


def rms_norm(values, gain_w):
    vals_f = values.astype(F32)
    inv_rms = lax.rsqrt(jnp.mean(vals_f * vals_f, axis=-1, keepdims=True) + EPS)
    return (vals_f * inv_rms * gain_w.astype(F32)).astype(BF16)


def rms_norm_grad(values, gain_w, d_out):
    vals_f = values.astype(F32)
    inv_rms = lax.rsqrt(jnp.mean(vals_f * vals_f, axis=-1, keepdims=True) + EPS)
    unit = vals_f * inv_rms
    d_f = d_out.astype(F32)
    d_gain = jnp.sum(d_f * unit, axis=0)
    d_unit = d_f * gain_w.astype(F32)
    d_vals = inv_rms * (d_unit - unit * jnp.mean(d_unit * unit, axis=-1, keepdims=True))
    return d_vals.astype(BF16), d_gain


LANES = 128


def lane_index(shape):
    return lax.broadcasted_iota(jnp.int32, shape, len(shape) - 1)


def swap_halves(tensor, head_dim):
    half = head_dim // 2
    cols = []
    for start in range(0, tensor.shape[ONE], LANES):
        col = tensor[:, start:start + LANES]
        first = (lane_index(col.shape) % head_dim) < half
        cols.append(jnp.where(first, pltpu.roll(col, LANES - half, 1), pltpu.roll(col, half, 1)))
    return jnp.concatenate(cols, axis=1)


def tile_lanes(table, width):
    return jnp.concatenate([table] * (width // LANES), axis=1)


def pick_heads(tensor, sources, head_dim):
    cols = []
    for out in range(0, len(sources), 2):
        parts = []
        for side in range(2):
            src = sources[out + side]
            col = tensor[:, (src // 2) * LANES:(src // 2 + 1) * LANES]
            parts.append(col if src % 2 == side else pltpu.roll(col, head_dim, 1))
        cols.append(jnp.where(lane_index(parts[ZERO].shape) < head_dim, parts[ZERO], parts[ONE]))
    return jnp.concatenate(cols, axis=1)


def group_orders(heads, kv_heads):
    q_group = heads // kv_heads
    to_group = [kv * q_group + g for g in range(q_group) for kv in range(kv_heads)]
    to_natural = [(h % q_group) * kv_heads + h // q_group for h in range(heads)]
    return to_group, to_natural


def stack_sides(tensor, col, q_group, kv_cols, head_dim):
    parts = []
    for side in range(2):
        for g in range(q_group):
            start = (g * kv_cols + col) * LANES
            part = tensor[:, start:start + LANES]
            keep = (lane_index(part.shape) < head_dim) == (side == 0)
            parts.append(jnp.where(keep, part, 0.0).astype(BF16))
    return jnp.concatenate(parts, axis=0)


def unstack_sides(stacked, tokens, q_group, head_dim):
    outs = []
    for g in range(q_group):
        low = stacked[g * tokens:(g + 1) * tokens]
        high = stacked[(q_group + g) * tokens:(q_group + g + 1) * tokens]
        outs.append(jnp.where(lane_index(low.shape) < head_dim, low, high))
    return outs


def probabilities(q_stack, k_col, seq_len, head_dim):
    tokens = k_col.shape[ZERO]
    scores = dot_nt(q_stack, k_col) * head_dim ** -0.5
    query_at = lax.broadcasted_iota(jnp.int32, scores.shape, 0) % tokens
    key_at = lax.broadcasted_iota(jnp.int32, scores.shape, 1)
    causal = (query_at >= key_at) & (query_at // seq_len == key_at // seq_len)
    scores = jnp.where(causal, scores, -1e30)
    weight = jnp.exp(scores - jnp.max(scores, axis=-1, keepdims=True))
    return weight / jnp.sum(weight, axis=-1, keepdims=True)


def attn_forward_kernel(heads, kv_heads, seq_len, tokens, x_ref, norm_a_ref, norm_f_ref, cos_ref, sin_ref, wq_ref, wk_ref, wv_ref, wo_ref, place_ref,
                        u_ref, hidden_ref, keep_ref, gift_ref, q_ref, k_ref, v_ref, mixed_ref):
    head_dim = wq_ref.shape[ZERO] // heads
    q_group = heads // kv_heads
    kv_cols = kv_heads // 2
    to_group, to_natural = group_orders(heads, kv_heads)
    cos_t, sin_t = cos_ref[...], sin_ref[...]
    normed = rms_norm(x_ref[...], norm_a_ref[...])
    d_model = normed.shape[ONE]
    keep_ref[:, :d_model] = normed
    gift_ref[:, :d_model] = normed

    def rotate(tensor):
        tens_f = tensor.astype(BF16).astype(F32)
        width = tensor.shape[ONE]
        return (tens_f * tile_lanes(cos_t, width) + swap_halves(tens_f, head_dim) * tile_lanes(sin_t, width)).astype(BF16)

    q_ref[...] = rotate(dot_nt(normed, wq_ref[...]))
    k_ref[...] = rotate(dot_nt(normed, wk_ref[...]))
    v_ref[...] = dot_nt(normed, wv_ref[...]).astype(BF16)

    def attend_slot(slot, _):
        span = pl.ds(pl.multiple_of(slot * tokens, tokens), tokens)
        query = pick_heads(q_ref[span, :].astype(F32), to_group, head_dim)
        mixed = [[None] * kv_cols for _ in range(q_group)]
        for col in range(kv_cols):
            lanes = slice(col * LANES, (col + 1) * LANES)
            prob = probabilities(stack_sides(query, col, q_group, kv_cols, head_dim), k_ref[span, lanes], seq_len, head_dim).astype(BF16)
            for g, part in enumerate(unstack_sides(dot_nn(prob, v_ref[span, lanes]), tokens, q_group, head_dim)):
                mixed[g][col] = part
        grouped = jnp.concatenate([part for row in mixed for part in row], axis=1)
        mixed_ref[span, :] = pick_heads(grouped, to_natural, head_dim).astype(BF16)
        return 0

    lax.fori_loop(0, x_ref.shape[ZERO] // tokens, attend_slot, 0)
    hidden = (x_ref[...].astype(F32) + dot_nn(mixed_ref[...], wo_ref[...])).astype(BF16)
    hidden_ref[...] = hidden
    u_ref[...] = rms_norm(hidden, norm_f_ref[...])
    half = mixed_ref.shape[ONE] // 2
    first = place_ref[ONE] == 0
    keep_ref[:, d_model:] = jnp.where(first, mixed_ref[:, :half], mixed_ref[:, half:])
    gift_ref[:, d_model:] = jnp.where(first, mixed_ref[:, half:], mixed_ref[:, :half])


def attn_forward(place, first, n_rows, x, norms, tables, weights, heads, kv_heads, seq_len, tokens):
    d_model = x.shape[ONE]
    base = first // n_rows
    wq, wk, _, _ = weights
    q_dim, kv_dim = wq.shape[ZERO], wk.shape[ZERO]

    def rows(width, start):
        return pl.BlockSpec((n_rows, width), lambda step: (start, ZERO))

    def whole(arr):
        return pl.BlockSpec(arr.shape, lambda step: (ZERO, ZERO))

    def out(width):
        return jax.ShapeDtypeStruct((n_rows, width), BF16)

    wide = d_model + q_dim // 2
    widths = (d_model, d_model, wide, wide, q_dim, kv_dim, kv_dim)
    tables = [jnp.tile(table, (n_rows // table.shape[ZERO], 1)) for table in tables]
    flops = 2 * n_rows * d_model * (2 * q_dim + 2 * kv_dim) * 2
    return pl.pallas_call(
        functools.partial(attn_forward_kernel, heads, kv_heads, seq_len, tokens),
        grid=(1,),
        in_specs=[rows(d_model, base)] + [whole(arr) for arr in (*norms, *tables, *weights)] + [pl.BlockSpec(memory_space=pltpu.SMEM)],
        out_specs=[rows(width, 0) for width in widths],
        out_shape=[out(width) for width in widths],
        scratch_shapes=[pltpu.VMEM((n_rows, q_dim), BF16)],
        compiler_params=pltpu.CompilerParams(vmem_limit_bytes=VMEM_BIG, dimension_semantics=('arbitrary',)),
        cost_estimate=pl.CostEstimate(flops=flops, bytes_accessed=40_000_000, transcendentals=0),
        name='attn_forward',
    )(x, *norms, *tables, *weights, place)


def attn_backward_kernel(heads, kv_heads, seq_len, tokens, x_ref, dy_ref, hidden_ref, q_ref, k_ref, v_ref, d_shared_ref, d_routed_ref,
                         norm_a_ref, norm_f_ref, cos_ref, sin_ref, wq_ref, wk_ref, wv_ref, wo_ref, place_ref, *refs):
    dx_ref, dh_ref, mine_ref, theirs_ref, g_norm_ref, d_mixed_s, dqkv_ref = refs[-7:]
    q_dim, kv_dim = wq_ref.shape[ZERO], wk_ref.shape[ZERO]
    head_dim = q_dim // heads
    q_group = heads // kv_heads
    kv_cols = kv_heads // 2
    to_group, to_natural = group_orders(heads, kv_heads)
    cos_t, sin_t = cos_ref[...], sin_ref[...]
    d_u = (d_routed_ref[...].astype(BF16).astype(F32) + d_shared_ref[...].astype(F32)).astype(BF16)
    d_hidden_u, g_norm_f = rms_norm_grad(hidden_ref[...], norm_f_ref[...], d_u)
    d_hidden = (dy_ref[...].astype(F32) + d_hidden_u.astype(F32)).astype(BF16)
    dh_ref[...] = d_hidden
    d_mixed_s[...] = dot_nt(d_hidden, wo_ref[...]).astype(BF16)

    def unrotate(tensor):
        tens_f = tensor.astype(BF16).astype(F32)
        width = tensor.shape[ONE]
        return tens_f * tile_lanes(cos_t, width) - swap_halves(tens_f, head_dim) * tile_lanes(sin_t, width)

    def attend_slot(slot, _):
        span = pl.ds(pl.multiple_of(slot * tokens, tokens), tokens)
        query = pick_heads(q_ref[span, :].astype(F32), to_group, head_dim)
        d_mixed = pick_heads(d_mixed_s[span, :].astype(F32), to_group, head_dim)
        d_query = [[None] * kv_cols for _ in range(q_group)]
        d_key, d_value = [], []
        for col in range(kv_cols):
            lanes = slice(col * LANES, (col + 1) * LANES)
            q_stack = stack_sides(query, col, q_group, kv_cols, head_dim)
            do_stack = stack_sides(d_mixed, col, q_group, kv_cols, head_dim)
            prob = probabilities(q_stack, k_ref[span, lanes], seq_len, head_dim)
            d_prob = dot_nt(do_stack, v_ref[span, lanes]).astype(BF16).astype(F32)
            d_score = prob * (d_prob - jnp.sum(d_prob * prob, axis=-1, keepdims=True)) * head_dim ** -0.5
            d_score = d_score.astype(BF16)
            for g, part in enumerate(unstack_sides(dot_nn(d_score, k_ref[span, lanes]), tokens, q_group, head_dim)):
                d_query[g][col] = part
            d_key.append(dot_tn(d_score, q_stack))
            d_value.append(dot_tn(prob.astype(BF16), do_stack))
        grouped = unrotate(jnp.concatenate([part for row in d_query for part in row], axis=1))
        dqkv_ref[span, :q_dim] = pick_heads(grouped, to_natural, head_dim).astype(BF16)
        dqkv_ref[span, q_dim:q_dim + kv_dim] = unrotate(jnp.concatenate(d_key, axis=1)).astype(BF16)
        dqkv_ref[span, q_dim + kv_dim:] = jnp.concatenate(d_value, axis=1).astype(BF16)
        return 0

    lax.fori_loop(0, x_ref.shape[ZERO] // tokens, attend_slot, 0)
    d_normed = dot_nn(dqkv_ref[:, :q_dim], wq_ref[...]) + dot_nn(dqkv_ref[:, q_dim:q_dim + kv_dim], wk_ref[...]) + dot_nn(dqkv_ref[:, q_dim + kv_dim:], wv_ref[...])
    d_x_norm, g_norm_a = rms_norm_grad(x_ref[...], norm_a_ref[...], d_normed.astype(BF16))
    dx_ref[...] = (d_hidden.astype(F32) + d_x_norm.astype(F32)).astype(BF16)
    width = mine_ref.shape[ONE]
    first = place_ref[ONE] == 0
    mine_ref[...] = jnp.where(first, dqkv_ref[:, :width], dqkv_ref[:, width:])
    theirs_ref[:, :width] = jnp.where(first, dqkv_ref[:, width:], dqkv_ref[:, :width])
    theirs_ref[:, width:] = d_hidden
    row = lax.broadcasted_iota(jnp.int32, g_norm_ref.shape[1:], 0)
    g_norm_ref[ZERO] = jnp.where(row == 0, g_norm_a[None], jnp.where(row == 1, g_norm_f[None], 0.0))


def attn_backward(place, first, n_rows, x, dy, group, group_at, d_routed, norms, tables, weights, heads, kv_heads, seq_len, tokens, done):
    all_tok, d_model = x.shape
    _, query, key, _, _ = group
    q_dim, kv_dim = query.shape[ONE], key.shape[ONE]
    half = q_dim // 2 + kv_dim
    base = first // n_rows

    def rows(width, start):
        return pl.BlockSpec((n_rows, width), lambda step: (start + step, ZERO))

    def whole(arr):
        return pl.BlockSpec(arr.shape, lambda step: (ZERO, ZERO))

    grouped = (d_model, q_dim, kv_dim, kv_dim, d_model)
    tables = [jnp.tile(table, (tokens // table.shape[ZERO], 1)) for table in tables]
    operands = [x, dy, *group, d_routed, *norms, *tables, *weights, place, *done]
    flops = 2 * n_rows * d_model * (2 * q_dim + 2 * kv_dim) * 2
    return pl.pallas_call(
        functools.partial(attn_backward_kernel, heads, kv_heads, seq_len, tokens),
        grid=(1,),
        in_specs=[rows(d_model, base)] * 2 + [rows(width, group_at) for width in grouped] + [rows(d_model, 0)] + [whole(arr) for arr in (*norms, *tables, *weights)]
        + [pl.BlockSpec(memory_space=pltpu.SMEM)] + [pl.BlockSpec(memory_space=pl.ANY)] * len(done),
        out_specs=[rows(width, base) for width in (d_model, d_model, half)] + [rows(half + d_model, 0), pl.BlockSpec((1, 8, d_model), lambda step: (step, ZERO, ZERO))],
        out_shape=[jax.ShapeDtypeStruct((all_tok, width), BF16) for width in (d_model, d_model, half)]
        + [jax.ShapeDtypeStruct((n_rows, half + d_model), BF16), jax.ShapeDtypeStruct((1, 8, d_model), F32)],
        scratch_shapes=[pltpu.VMEM((n_rows, q_dim), BF16), pltpu.VMEM((n_rows, 2 * half), BF16)],
        input_output_aliases={len(operands) - len(done) + idx: idx for idx in range(len(done))},
        compiler_params=pltpu.CompilerParams(vmem_limit_bytes=VMEM_BIG, dimension_semantics=('arbitrary',)),
        cost_estimate=pl.CostEstimate(flops=flops, bytes_accessed=30_000_000, transcendentals=0),
        name='attn_backward',
    )(*operands)


def shared_kernel(u_ref, hidden_ref, dy_ref, wg_ref, wu_ref, wd_ref, base_ref, d_shared_ref):
    u, dy = u_ref[...], dy_ref[...]
    gate_f = dot_nn(u, wg_ref[...]).astype(BF16).astype(F32)
    up_f = dot_nn(u, wu_ref[...]).astype(BF16).astype(F32)
    sig_gate = jax.nn.sigmoid(gate_f)
    silu_gate = gate_f * sig_gate
    inner = (silu_gate * up_f).astype(BF16)
    base_ref[...] = hidden_ref[...].astype(F32) + dot_nn(inner, wd_ref[...])
    d_inner = dot_nt(dy, wd_ref[...]).astype(BF16).astype(F32)
    d_gate = (d_inner * up_f * sig_gate * (1.0 + gate_f * (1.0 - sig_gate))).astype(BF16)
    d_up = (d_inner * silu_gate).astype(BF16)
    from_gate = dot_nt(d_gate, wg_ref[...]).astype(BF16).astype(F32)
    from_up = dot_nt(d_up, wu_ref[...]).astype(BF16).astype(F32)
    d_shared_ref[...] = (from_gate + from_up).astype(BF16)


def shared_expert(u, hidden, dy, chunks_before, s_gate, s_up, s_down):
    n_rows, d_model = u.shape
    d_ff = s_gate.shape[ONE]
    dy_at = chunks_before * (dy.shape[ZERO] // CHUNKS) // n_rows

    def rows(start):
        return pl.BlockSpec((n_rows, d_model), lambda step: (start, ZERO))

    def whole(arr):
        return pl.BlockSpec(arr.shape, lambda step: (ZERO, ZERO))

    return pl.pallas_call(
        shared_kernel,
        grid=(1,),
        in_specs=[rows(0), rows(0), rows(dy_at)] + [whole(arr) for arr in (s_gate, s_up, s_down)],
        out_specs=[rows(0)] * 2,
        out_shape=[jax.ShapeDtypeStruct((n_rows, d_model), F32), jax.ShapeDtypeStruct((n_rows, d_model), BF16)],
        compiler_params=pltpu.CompilerParams(vmem_limit_bytes=VMEM_BIG, dimension_semantics=('arbitrary',)),
        cost_estimate=pl.CostEstimate(flops=12 * n_rows * d_model * d_ff, bytes_accessed=25_000_000, transcendentals=0),
        name='shared_expert',
    )(u, hidden, dy, s_gate, s_up, s_down)


def shared_grad_kernel(place_ref, u_a, u_b, dy_a, dy_b, wg_ref, wu_ref, wd_ref, *refs):
    g_in_ref, g_down_ref, d_both = refs[-3:]
    half = wg_ref.shape[ONE]

    @pl.when(pl.program_id(0) == 0)
    def _begin():
        for idx, out in enumerate((g_in_ref, g_down_ref)):
            out[...] = refs[idx][...] if len(refs) > 3 else jnp.zeros_like(out)

    u = jnp.concatenate([u_a[ZERO], u_b[ZERO]], axis=0)
    dy = jnp.concatenate([dy_a[ZERO], dy_b[ZERO]], axis=0)
    gate_f = dot_nn(u, wg_ref[...]).astype(BF16).astype(F32)
    up_f = dot_nn(u, wu_ref[...]).astype(BF16).astype(F32)
    sig_gate = jax.nn.sigmoid(gate_f)
    silu_gate = gate_f * sig_gate
    inner = (silu_gate * up_f).astype(BF16)
    d_inner = dot_nt(dy, wd_ref[...]).astype(BF16).astype(F32)
    d_both[:, :half] = (d_inner * up_f * sig_gate * (1.0 + gate_f * (1.0 - sig_gate))).astype(BF16)
    d_both[:, half:] = (d_inner * silu_gate).astype(BF16)
    g_in_ref[...] += dot_tn(u, d_both[...])
    g_down_ref[...] += dot_tn(inner, dy)


def shared_grads(place, u_pair, dy_all, rows, n_chunks, s_gate, s_up, s_down, done):
    d_model, d_ff = s_gate.shape
    half = d_ff // 2
    n_pairs = u_pair[ZERO].shape[ZERO]

    def dy_spec(other):
        if isinstance(dy_all, tuple):
            return pl.BlockSpec((1, rows, d_model), lambda step, place: (step % n_pairs, step // n_pairs, ZERO))

        def index(step, place):
            core = 1 - place[ONE] if other else place[ONE]
            return (2 * jnp.bitwise_xor(step % n_pairs, place[ZERO]) + core, step // n_pairs, 0)

        return pl.BlockSpec((1, rows, d_model), index)

    u_spec = pl.BlockSpec((1, rows, d_model), lambda step, place: (step % n_pairs, step // n_pairs, ZERO))
    wide_in = pl.BlockSpec((d_model, half), lambda step, place: (ZERO, place[ONE]))
    tall_in = pl.BlockSpec((half, d_model), lambda step, place: (place[ONE], ZERO))
    sums = [pl.BlockSpec((d_model, d_ff), lambda step, place: (ZERO, ZERO)), pl.BlockSpec((half, d_model), lambda step, place: (ZERO, ZERO))]
    flops = 12 * n_chunks * n_pairs * 2 * rows * d_model * half
    return pl.pallas_call(
        shared_grad_kernel,
        grid_spec=pltpu.PrefetchScalarGridSpec(
            num_scalar_prefetch=1,
            grid=(n_chunks * n_pairs,),
            in_specs=[u_spec, u_spec, dy_spec(False), dy_spec(True), wide_in, wide_in, tall_in] + sums[:len(done)],
            out_specs=sums,
            scratch_shapes=[pltpu.VMEM((2 * rows, d_ff), BF16)],
        ),
        out_shape=[jax.ShapeDtypeStruct((d_model, d_ff), F32), jax.ShapeDtypeStruct((half, d_model), F32)],
        input_output_aliases={8 + idx: idx for idx in range(len(done))},
        compiler_params=pltpu.CompilerParams(vmem_limit_bytes=VMEM_BIG, dimension_semantics=('arbitrary',)),
        cost_estimate=pl.CostEstimate(flops=flops, bytes_accessed=25_000_000, transcendentals=0),
        name='shared_grads',
    )(place, *u_pair, *(dy_all if isinstance(dy_all, tuple) else (dy_all, dy_all)), s_gate, s_up, s_down, *done)


def dense_grad_kernel(width, n_groups, n_chunks, kept, place_ref, *refs):
    keeps, gifts, rest = refs[:n_groups], refs[n_groups:2 * n_groups], refs[2 * n_groups:]
    mine, d_hidden, twins = rest[ZERO], rest[ONE], rest[2:2 + n_chunks]
    out_a, out_b, d_qkv, normed, mixed, d_hid, sems = rest[2 + n_chunks:]
    half, d_model = d_qkv.shape[ONE], normed.shape[ONE]
    step = pl.program_id(0)
    n_own = mine.shape[ZERO]
    loads, at = [], 0
    for ref in (*keeps, *gifts):
        span = pl.ds(at, ref.shape[ZERO])
        loads.append((0, ref.at[:, pl.ds(0, d_model)], normed.at[span]))
        loads.append((1, ref.at[:, pl.ds(d_model, ref.shape[ONE] - d_model)], mixed.at[span]))
        at += ref.shape[ZERO]
    loads += [(0, mine, d_qkv.at[pl.ds(0, n_own)]), (1, d_hidden, d_hid.at[pl.ds(0, n_own)])]
    for idx, ref in enumerate(twins):
        span = pl.ds(n_own + idx * ref.shape[ZERO], ref.shape[ZERO])
        loads.append((0, ref.at[:, pl.ds(0, half)], d_qkv.at[span]))
        loads.append((1, ref.at[:, pl.ds(half, d_model)], d_hid.at[span]))
    copies = [(late, pltpu.make_async_copy(src, dst, sems.at[idx])) for idx, (late, src, dst) in enumerate(loads)]

    @pl.when(step == 0)
    def _load():
        for _, copy in copies:
            copy.start()
        for late, copy in copies:
            if not late:
                copy.wait()

    per_half = pl.num_programs(0) // 2

    @pl.when(step == per_half)
    def _load_rest():
        for late, copy in copies:
            if late:
                copy.wait()

    for part, out_ref in enumerate((out_a, out_b)):
        bit = place_ref[ZERO] % 2 if part == 0 else place_ref[ZERO] // 2
        block = 2 * per_half * part + per_half * (bit if kept else 1 - bit) + step % per_half
        at = pl.multiple_of(block * width, LANES)

        @pl.when((step // per_half == part) & (at < half))
        def _qkv(at=at, out_ref=out_ref):
            out_ref[...] = dot_tn(d_qkv[:, pl.ds(at, width)], normed[...])

        if part == 1:
            @pl.when((step // per_half == part) & (at >= half))
            def _out(at=at, out_ref=out_ref):
                out_ref[...] = dot_tn(mixed[:, pl.ds(pl.multiple_of(at - half, LANES), width)], d_hid[...])


def dense_grads(place, kept, keeps, gifts, mine, d_hidden, twins, width):
    n_own, half = mine.shape
    d_model = d_hidden.shape[ONE]
    mixed_half = keeps[ZERO].shape[ONE] - d_model
    n_out = half + mixed_half
    assert n_out // 2 <= half and n_out % (4 * width) == 0 and half % width == 0
    n_in = 2 * len(keeps) + 2 + len(twins)
    n_loads = 4 * len(keeps) + 2 + 2 * len(twins)
    per_half = n_out // 4 // width
    return pl.pallas_call(
        functools.partial(dense_grad_kernel, width, len(keeps), len(twins), kept),
        grid=(2 * per_half,),
        in_specs=[pl.BlockSpec(memory_space=pltpu.SMEM)] + [pl.BlockSpec(memory_space=pl.ANY)] * n_in,
        out_specs=[pl.BlockSpec((width, d_model), lambda step: (jnp.minimum(step, per_half - ONE), ZERO)),
                   pl.BlockSpec((width, d_model), lambda step: (jnp.maximum(step - per_half, ZERO), ZERO))],
        out_shape=[jax.ShapeDtypeStruct((n_out // 4, d_model), F32)] * 2,
        scratch_shapes=[pltpu.VMEM((2 * n_own, cols), BF16) for cols in (half, d_model, mixed_half, d_model)] + [pltpu.SemaphoreType.DMA((n_loads,))],
        compiler_params=pltpu.CompilerParams(vmem_limit_bytes=VMEM_BIG, dimension_semantics=('arbitrary',)),
        cost_estimate=pl.CostEstimate(flops=2 * n_own * n_out * d_model, bytes_accessed=30_000_000, transcendentals=0),
        name='dense_grads',
    )(place, *keeps, *gifts, mine, d_hidden, *twins)


def exchange(value, mask):
    return lax.ppermute(value, 'ep', [(idx, idx ^ mask) for idx in range(N_DEV)])


def gather_rows(own):
    half = own.shape[ZERO] // 2
    from_x = exchange(own, 2)
    from_y = exchange(own, 4)
    far_a = exchange(from_y[:half], 2)
    far_b = exchange(from_x[half:], 4)
    same = jnp.concatenate([own, from_x, from_y, far_a, far_b], axis=0).reshape(4, *own.shape)
    return same, exchange(same, 1)


def reduce_rows(sums):
    same, other = sums
    half = same.shape[ONE] // 2
    twin = exchange(other, 1)
    via_x = exchange(same[3, :half] + twin[3, :half], 2)
    via_y = exchange(same[3, half:] + twin[3, half:], 4)
    to_x = same[ONE] + twin[ONE] + jnp.pad(via_y, ((half, 0), (0, 0)))
    to_y = same[2] + twin[2] + jnp.pad(via_x, ((0, half), (0, 0)))
    return same[ZERO] + twin[ZERO] + exchange(to_x, 2) + exchange(to_y, 4)


def halves(value, bit):
    size = value.shape[ZERO] // 2
    keep = lax.dynamic_slice_in_dim(value, bit * size, size)
    return keep, lax.dynamic_slice_in_dim(value, (1 - bit) * size, size)


def join(mine, theirs, bit, axis=0):
    return jnp.where(bit == 0, jnp.concatenate([mine, theirs], axis=axis), jnp.concatenate([theirs, mine], axis=axis))


def assemble_kernel(place_ref, *refs):
    pieces, outs, sems = refs[:8], refs[8:12], refs[12]
    size = pieces[ZERO].shape[ZERO]
    out_half = outs[3].shape[ZERO] // 2
    qkv_half = 4 * size - out_half
    bits = (place_ref[ZERO] % 2, place_ref[ZERO] // 2)
    runs = {}
    for at_core in range(2):
        runs[at_core] = [(qkv_half, qkv_half + out_half, 3, at_core * out_half)]
        begin = 0
        for idx, out in enumerate(outs[:3]):
            low, high = max(begin, at_core * qkv_half), min(begin + out.shape[ZERO], (at_core + 1) * qkv_half)
            if low < high:
                runs[at_core].append((low - at_core * qkv_half, high - at_core * qkv_half, idx, low - begin))
            begin += out.shape[ZERO]
    copies = []
    for idx, piece in enumerate(pieces):
        side, half, late = idx // 4, idx // 2 % 2, idx % 2
        core = place_ref[ONE] if side == 0 else 1 - place_ref[ONE]
        sub = bits[half] if late == 0 else 1 - bits[half]
        for at_core in range(2):
            for at_sub in range(2):
                start = (2 * half + at_sub) * size
                parts = []
                for low, high, out, into in runs[at_core]:
                    begin, end = max(start, low), min(start + size, high)
                    if begin < end:
                        source = piece.at[pl.ds(begin - start, end - begin)]
                        parts.append(pltpu.make_async_copy(source, outs[out].at[pl.ds(into + begin - low, end - begin)], sems.at[idx, len(parts)]))
                copies.append(((core == at_core) & (sub == at_sub), parts))
    for begin in (True, False):
        for here, parts in copies:
            @pl.when(here)
            def _move(parts=parts):
                for part in parts:
                    if begin:
                        part.start()
                    else:
                        part.wait()


def assemble(place, pieces, heights):
    n_cols = pieces[ZERO].shape[ONE]
    return pl.pallas_call(
        assemble_kernel,
        in_specs=[pl.BlockSpec(memory_space=pltpu.SMEM)] + [pl.BlockSpec(memory_space=pltpu.VMEM)] * 8,
        out_specs=[pl.BlockSpec(memory_space=pl.ANY)] * 4,
        out_shape=[jax.ShapeDtypeStruct((height, n_cols), F32) for height in heights],
        scratch_shapes=[pltpu.SemaphoreType.DMA((8, 4))],
        compiler_params=pltpu.CompilerParams(vmem_limit_bytes=VMEM_BIG),
        cost_estimate=pl.CostEstimate(flops=10_000_000, bytes_accessed=50_000_000, transcendentals=0),
        name='assemble',
    )(place, *pieces)


def all_reduce_rows(place, kept, sent, heights):
    bits = {2: place[ZERO] % 2, 4: place[ZERO] // 2}
    mine, twins = [], []
    for keep, send, (one, two) in ((kept[ZERO], sent[ZERO], (2, 4)), (kept[ONE], sent[ONE], (4, 2))):
        part = keep + exchange(send, one)
        keep, send = halves(part, bits[two])
        part = keep + exchange(send, two)
        part = join(part, exchange(part, two), bits[two])
        late = exchange(part, one)
        mine += [part, late]
        twins += [exchange(part, 1), exchange(late, 1)]
    return assemble(place, mine + twins, heights)


def small_all_reduce(value):
    for mask in (1, 2, 4):
        value = value + exchange(value, mask)
    return value


def choice_keys(choice_ids, n_exp):
    _, top_k, tokens = choice_ids.shape
    same = choice_ids[:, None, :, :] == jnp.arange(n_exp)[None, :, None, None]
    count = jnp.sum(same, axis=2, dtype=F32)
    before = (jnp.arange(tokens)[:, None] < jnp.arange(tokens)[None, :]).astype(BF16)
    prefix = jnp.einsum('set,tu->seu', count.astype(BF16), before, preferred_element_type=F32)
    rank = jnp.sum(jnp.where(same, prefix[:, :, None, :], 0.0), axis=1)
    earlier = jnp.arange(top_k)[:, None] > jnp.arange(top_k)[None, :]
    repeat = (choice_ids[:, :, None, :] == choice_ids[:, None, :, :]) & earlier[None, :, :, None]
    rank = rank + jnp.sum(repeat, axis=2, dtype=F32)
    return choice_ids.astype(F32) * KEY_STRIDE + rank


def row_plans(seg_rows):
    return ((512, 512), (640, 320), (seg_rows, seg_rows // 2))


def plan_of(total, plans, index):
    low = plans[index - 1][ZERO] if index else -1
    return (total > low) & (total <= plans[index][ZERO])


def expert_kernel(n_segs, local_e, pair_rows, part, place_ref, offs_ref, keys_a, keys_b, gates_a, gates_b, u_a, u_b, dy_a, dy_b,
                  wg_ref, wu_ref, wd_ref, *refs):
    y_ref, du_a, du_b, dgate_ref, dup_ref, inner_ref, rows_hbm, drows_hbm, pick, pick_g, buf_u, buf_d, sems = refs[-13:]
    step = pl.program_id(0)
    tokens = u_a.shape[ONE]
    d_model = u_a.shape[2]
    d_ff = wg_ref.shape[2]
    top_k = keys_a.shape[2]
    plans = row_plans(n_segs * pair_rows)

    def offset(exp, seg):
        return pl.multiple_of(offs_ref[exp, seg], 16)

    @pl.when(step < n_segs)
    def _gather():
        seg = step
        keys = jnp.concatenate([keys_a[ZERO, ZERO], keys_b[ZERO, ZERO]], axis=1)
        gates = jnp.concatenate([gates_a[ZERO, ZERO], gates_b[ZERO, ZERO]], axis=1)
        for exp in range(local_e):
            row = lax.broadcasted_iota(jnp.int32, (pair_rows, 2 * tokens), 0).astype(F32) + exp * KEY_STRIDE
            chosen = jnp.zeros((pair_rows, 2 * tokens), F32)
            weight = jnp.zeros((pair_rows, 2 * tokens), F32)
            for choice in range(top_k):
                hit = keys[choice:choice + 1, :] == row
                chosen = jnp.where(hit, 1.0, chosen)
                weight = jnp.where(hit, gates[choice:choice + 1, :], weight)
            pick[seg, pl.ds(exp * pair_rows, pair_rows), :] = chosen.astype(BF16)
            pick_g[seg, pl.ds(exp * pair_rows, pair_rows), :] = weight.astype(BF16)
        for source, picks, buf in (((u_a, u_b), pick, buf_u), ((dy_a, dy_b), pick_g, buf_d)):
            for lane in range(0, d_model, d_ff):
                lanes = slice(lane, lane + d_ff)
                got = dot_nn(picks[seg], jnp.concatenate([source[ZERO][ZERO, :, lanes], source[ONE][ZERO, :, lanes]], axis=0)).astype(BF16)
                for exp in range(local_e):
                    buf[exp, pl.ds(offset(exp, seg), pair_rows), lanes] = got[exp * pair_rows:(exp + 1) * pair_rows]

    @pl.when(step == n_segs - 1)
    def _clear_tails():
        for exp in range(local_e):
            total = offs_ref[exp, n_segs]
            start = offs_ref[exp, n_segs - 1] + pair_rows
            limit = jnp.int32(0)
            for index in range(len(plans)):
                limit = jnp.where(plan_of(total, plans, index), plans[index][ZERO], limit)

            def clear(block, _):
                at = pl.multiple_of(start + block * 16, 16)
                buf_u[exp, pl.ds(at, 16), :] = jnp.zeros((16, d_model), BF16)
                buf_d[exp, pl.ds(at, 16), :] = jnp.zeros((16, d_model), BF16)
                return 0

            lax.fori_loop(0, jnp.maximum(limit - start, 0) // 16, clear, 0)

    def run_rows(exp, start, count):
        span = slice(start, start + count)
        gate_f = dot_nn(buf_u[exp, span, :], wg_ref[ZERO]).astype(BF16).astype(F32)
        up_f = dot_nn(buf_u[exp, span, :], wu_ref[ZERO]).astype(BF16).astype(F32)
        sig_gate = jax.nn.sigmoid(gate_f)
        silu_gate = gate_f * sig_gate
        inner_ref[ZERO, ZERO, span, :] = (silu_gate * up_f).astype(BF16)
        d_inner = dot_nt(buf_d[exp, span, :], wd_ref[ZERO]).astype(BF16).astype(F32)
        dgate_ref[ZERO, ZERO, span, :] = (d_inner * up_f * sig_gate * (1.0 + gate_f * (1.0 - sig_gate))).astype(BF16)
        dup_ref[ZERO, ZERO, span, :] = (d_inner * silu_gate).astype(BF16)

    def finish_rows(exp, start, count):
        span = slice(start, start + count)
        for lane in range(0, d_model, d_ff):
            lanes = slice(lane, lane + d_ff)
            buf_u[exp, span, lanes] = dot_nn(inner_ref[ZERO, ZERO, span, :], wd_ref[ZERO, :, lanes]).astype(BF16)
            from_gate = dot_nt(dgate_ref[ZERO, ZERO, span, :], wg_ref[ZERO, lanes, :]).astype(BF16).astype(F32)
            from_up = dot_nt(dup_ref[ZERO, ZERO, span, :], wu_ref[ZERO, lanes, :]).astype(BF16).astype(F32)
            buf_d[exp, span, lanes] = (from_gate + from_up).astype(BF16)

    @pl.when((step >= n_segs) & (step < n_segs + local_e))
    def _experts():
        exp = step - n_segs
        total = offs_ref[exp, n_segs]
        for index, (count, per_pass) in enumerate(plans):
            @pl.when(plan_of(total, plans, index))
            def _run(count=count, per_pass=per_pass):
                saves = [pltpu.make_async_copy(buf.at[exp, pl.ds(0, count)], hbm.at[part, exp, pl.ds(0, count)], sems.at[idx])
                         for idx, (buf, hbm) in enumerate(((buf_u, rows_hbm), (buf_d, drows_hbm)))]
                for save in saves:
                    save.start()
                for start in range(0, count, per_pass):
                    run_rows(exp, start, per_pass)
                for save in saves:
                    save.wait()
                for start in range(0, count, per_pass):
                    finish_rows(exp, start, per_pass)

    @pl.when(step >= n_segs + local_e)
    def _combine():
        seg = step - (n_segs + local_e)
        core = place_ref[ONE]
        for lane in range(0, d_model, d_ff):
            lanes = slice(lane, lane + d_ff)
            results = jnp.concatenate([buf_u[exp, pl.ds(offset(exp, seg), pair_rows), lanes] for exp in range(local_e)], axis=0)
            y_sum = dot_tn(pick_g[seg], results)
            y_ref[core, :, lanes] = y_sum[:tokens]
            y_ref[1 - core, :, lanes] = y_sum[tokens:]
            d_rows = jnp.concatenate([buf_d[exp, pl.ds(offset(exp, seg), pair_rows), lanes] for exp in range(local_e)], axis=0)
            du_sum = dot_tn(pick[seg], d_rows)
            du_a[ZERO, :, lanes] = du_sum[:tokens]
            du_b[ZERO, :, lanes] = du_sum[tokens:]


def route_kernel(n_pairs, n_slots, local_e, chunk, index_ref, *refs):
    table_refs, (keys_ref, gates_ref, offs_ref) = refs[:-3], refs[-3:]
    first_key = (index_ref[ZERO] * (local_e * KEY_STRIDE)).astype(F32)
    n_segs = chunk * n_pairs
    rows = {}
    for pair in range(n_pairs):
        sides = [table_refs[2 * pair + side][ZERO] - first_key for side in range(2)]
        shifted = sides[ONE]
        for exp in range(local_e):
            counts = []
            for keys in sides:
                mine = (keys >= exp * KEY_STRIDE) & (keys < (exp + 1) * KEY_STRIDE)
                by_lane = jnp.sum(jnp.where(mine, 1.0, 0.0), axis=1, keepdims=True)
                counts.append(jnp.sum(by_lane, axis=2, keepdims=True))
            second = (sides[ONE] >= exp * KEY_STRIDE) & (sides[ONE] < (exp + 1) * KEY_STRIDE)
            shifted = jnp.where(second, sides[ONE] + counts[ZERO], shifted)
            rows[pair, exp] = jnp.ceil((counts[ZERO] + counts[ONE]) * (1.0 / 16)) * 16
        keys_ref[2 * pair] = sides[ZERO]
        keys_ref[2 * pair + 1] = shifted
        for side in range(2):
            gates_ref[2 * pair + side] = table_refs[2 * pair + side][ONE]
    lane = lax.broadcasted_iota(jnp.int32, (1, LANES), 1)
    for part in range(n_slots // chunk):
        for exp in range(local_e):
            at = jnp.zeros((1, 1), F32)
            line = jnp.zeros((1, LANES), F32)
            for seg in range(n_segs + 1):
                line = jnp.where(lane == seg, at, line)
                if seg < n_segs:
                    at = at + rows[seg % n_pairs, exp][part * chunk + seg // n_pairs]
            offs_ref[part, exp:exp + 1, :] = line.astype(jnp.int32)


def route_tables(index, tables, local_e, chunk):
    n_dev = len(tables)
    _, n_slots, top_k, tokens = tables[ZERO].shape
    whole = jax.ShapeDtypeStruct((n_dev, n_slots, top_k, tokens), F32)
    return pl.pallas_call(
        functools.partial(route_kernel, n_dev // 2, n_slots, local_e, chunk),
        in_specs=[pl.BlockSpec(memory_space=pltpu.SMEM)] + [pl.BlockSpec(memory_space=pltpu.VMEM)] * n_dev,
        out_specs=[pl.BlockSpec(memory_space=pltpu.VMEM)] * 3,
        out_shape=[whole, whole, jax.ShapeDtypeStruct((n_slots // chunk, local_e, LANES), jnp.int32)],
        cost_estimate=pl.CostEstimate(flops=10_000_000, bytes_accessed=1_000_000, transcendentals=0),
        name='route_tables',
    )(index, *tables)


def expert_pass(place, offs, keys, gates, u_pair, u_at, dy_all, dy_at, weights, saved, cap, tokens, part, n_parts):
    e_gate, e_up, e_down = weights
    n_dev, all_slots, top_k, _ = keys.shape
    local_e, d_model, d_ff = e_gate.shape
    n_pairs = n_dev // 2
    chunk = all_slots // n_parts
    n_segs = chunk * n_pairs
    pair_rows = 2 * cap
    exp_rows = n_segs * pair_rows
    last = n_segs + local_e

    def seg_in(step):
        return jnp.minimum(step, n_segs - 1)

    def expert_of(step):
        return jnp.clip(step - n_segs, 0, local_e - 1)

    def seg_out(step):
        return jnp.maximum(step - last, 0)

    def device(pair, place, other):
        core = 1 - place[ONE] if other else place[ONE]
        return 2 * jnp.bitwise_xor(pair, place[ZERO]) + core

    def route_spec(other):
        return pl.BlockSpec((1, 1, top_k, tokens), lambda step, *_: (2 * (seg_in(step) % n_pairs) + other, part * chunk + seg_in(step) // n_pairs, ZERO, ZERO))

    def dy_spec(other):
        if isinstance(dy_all, tuple):
            return pl.BlockSpec((1, tokens, d_model), lambda step, *_: (seg_in(step) % n_pairs, dy_at + seg_in(step) // n_pairs, ZERO))
        return pl.BlockSpec((1, tokens, d_model), lambda step, place, _: (device(seg_in(step) % n_pairs, place, other), dy_at + seg_in(step) // n_pairs, ZERO))

    u_spec = pl.BlockSpec((1, tokens, d_model), lambda step, *_: (seg_in(step) % n_pairs, u_at + seg_in(step) // n_pairs, ZERO))
    y_out = pl.BlockSpec((2, tokens, d_model), lambda step, place, _: (jnp.bitwise_xor(seg_out(step) % n_pairs, place[ZERO]), seg_out(step) // n_pairs, ZERO))
    du_out = pl.BlockSpec((1, tokens, d_model), lambda step, *_: (seg_out(step) % n_pairs, seg_out(step) // n_pairs, ZERO))
    wide = pl.BlockSpec((1, d_model, d_ff), lambda step, *_: (expert_of(step), ZERO, ZERO))
    tall = pl.BlockSpec((1, d_ff, d_model), lambda step, *_: (expert_of(step), ZERO, ZERO))
    save_f = pl.BlockSpec((1, 1, exp_rows, d_ff), lambda step, *_: (part, expert_of(step), ZERO, ZERO))
    anywhere = pl.BlockSpec(memory_space=pl.ANY)
    y_sum = jax.ShapeDtypeStruct((n_dev, chunk * tokens, d_model), F32)
    du_sum = jax.ShapeDtypeStruct((n_pairs, chunk * tokens, d_model), F32)
    saved_d = jax.ShapeDtypeStruct((n_parts, local_e, exp_rows, d_model), BF16)
    saved_f = jax.ShapeDtypeStruct((n_parts, local_e, exp_rows, d_ff), BF16)
    in_specs = [route_spec(False), route_spec(True), route_spec(False), route_spec(True), u_spec, u_spec, dy_spec(False), dy_spec(True), wide, wide, tall]
    operands = [keys, keys, gates, gates, *u_pair, *(dy_all if isinstance(dy_all, tuple) else (dy_all, dy_all)), e_gate, e_up, e_down]
    aliases = {}
    if saved is not None:
        aliases = {2 + len(operands) + idx: 3 + idx for idx in range(5)}
        in_specs += [anywhere] * 5
        operands += saved
    flops = n_segs * pair_rows * local_e * (12 * d_model * d_ff + 8 * 2 * tokens * d_model) // 2
    out = pl.pallas_call(
        functools.partial(expert_kernel, n_segs, local_e, pair_rows, part),
        grid_spec=pltpu.PrefetchScalarGridSpec(
            num_scalar_prefetch=2,
            grid=(last + n_segs,),
            in_specs=in_specs,
            out_specs=[y_out, du_out, du_out, save_f, save_f, save_f, anywhere, anywhere],
            scratch_shapes=[
                pltpu.VMEM((n_segs, local_e * pair_rows, 2 * tokens), BF16),
                pltpu.VMEM((n_segs, local_e * pair_rows, 2 * tokens), BF16),
                pltpu.VMEM((local_e, exp_rows, d_model), BF16),
                pltpu.VMEM((local_e, exp_rows, d_model), BF16),
                pltpu.SemaphoreType.DMA((2,)),
            ],
        ),
        out_shape=[y_sum, du_sum, du_sum, saved_f, saved_f, saved_f, saved_d, saved_d],
        input_output_aliases=aliases,
        compiler_params=pltpu.CompilerParams(vmem_limit_bytes=VMEM_BIG, dimension_semantics=('arbitrary',)),
        cost_estimate=pl.CostEstimate(flops=flops, bytes_accessed=120_000_000, transcendentals=0),
        name='expert_pass',
    )(place, offs, *operands)
    return out[ZERO], (out[ONE], out[2]), list(out[3:])


def expert_grad_kernel(base, plans, totals_ref, dgate_ref, dup_ref, inner_ref, rows_ref, drows_ref, *refs):
    whole, sums, rest = refs[:5], refs[-10:-7], refs[-7:]
    extra, sems = rest[:5], rest[5]
    part = pl.program_id(1)
    exp = base + pl.program_id(0)
    total = totals_ref[part, exp]

    def products(blocks):
        dgate, dup, inner, rows, drows = blocks
        return ((rows, dgate), (rows, dup), (inner, drows))

    near = [ref.at[ZERO, ZERO] for ref in (dgate_ref, dup_ref, inner_ref, rows_ref, drows_ref)]

    @pl.when(part == 0)
    def _first():
        for out, (lhs, rhs) in zip(sums, products(near)):
            out[ZERO] = dot_tn(lhs[...], rhs[...])

    @pl.when(part > 0)
    def _next():
        for out, (lhs, rhs) in zip(sums, products(near)):
            out[ZERO] += dot_tn(lhs[...], rhs[...])

    low = plans[ZERO][ZERO]
    for count, _ in plans[1:]:
        @pl.when(total > low)
        def _more(low=low, count=count):
            far = [buf.at[pl.ds(0, count - low)] for buf in extra]
            copies = [pltpu.make_async_copy(ref.at[part, exp, pl.ds(low, count - low)], buf, sems.at[idx]) for idx, (ref, buf) in enumerate(zip(whole, far))]
            for copy in copies:
                copy.start()
            for copy in copies:
                copy.wait()
            for out, (lhs, rhs) in zip(sums, products(far)):
                out[ZERO] += dot_tn(lhs[...], rhs[...])

        low = count


def expert_grads(totals, saved, experts, done):
    parts, local_e, n_rows, d_model = saved[3].shape
    d_ff = saved[ZERO].shape[3]
    base, count = experts
    plans = row_plans(n_rows)
    near = plans[ZERO][ZERO]
    far = max(high - low for (low, _), (high, _) in zip(plans, plans[1:]))
    in_d = pl.BlockSpec((1, 1, near, d_model), lambda exp, part, _: (part, base + exp, ZERO, ZERO))
    in_f = pl.BlockSpec((1, 1, near, d_ff), lambda exp, part, _: (part, base + exp, ZERO, ZERO))
    wide = pl.BlockSpec((1, d_model, d_ff), lambda exp, part, _: (base + exp, ZERO, ZERO))
    tall = pl.BlockSpec((1, d_ff, d_model), lambda exp, part, _: (base + exp, ZERO, ZERO))
    anywhere = pl.BlockSpec(memory_space=pl.ANY)
    flops = 6 * parts * count * near * d_model * d_ff
    return pl.pallas_call(
        functools.partial(expert_grad_kernel, base, plans),
        grid_spec=pltpu.PrefetchScalarGridSpec(
            num_scalar_prefetch=1,
            grid=(count, parts),
            in_specs=[in_f, in_f, in_f, in_d, in_d] + [anywhere] * (5 + len(done)),
            out_specs=[wide, wide, tall],
            scratch_shapes=[pltpu.VMEM((far, width), BF16) for width in (d_ff, d_ff, d_ff, d_model, d_model)] + [pltpu.SemaphoreType.DMA((5,)), pltpu.SMEM((1,), jnp.int32)],
        ),
        out_shape=[jax.ShapeDtypeStruct((local_e, d_model, d_ff), F32)] * 2 + [jax.ShapeDtypeStruct((local_e, d_ff, d_model), F32)],
        input_output_aliases={11 + idx: idx for idx in range(len(done))},
        compiler_params=pltpu.CompilerParams(vmem_limit_bytes=VMEM_BIG, dimension_semantics=('arbitrary', 'arbitrary')),
        cost_estimate=pl.CostEstimate(flops=flops, bytes_accessed=30_000_000 * count, transcendentals=0),
        name='expert_grads',
    )(totals, *saved, *saved, *done)


def solution(mesh):
    n_ep = mesh.shape['ep']
    assert n_ep == N_DEV

    def device_body(x_in, dy_in, expert_id, gate_vals, norm_attn, w_query, w_key, w_value, w_out, norm_ffn, s_gate, s_up, s_down, e_gate, e_up, e_down):
        n_slots, n_seq, seq_len, d_model = x_in.shape
        heads, head_dim = w_query.shape[2:]
        kv_heads = w_key.shape[2]
        top_k = expert_id.shape[-1]
        local_e = e_gate.shape[ONE]
        n_exp = local_e * n_ep
        tokens = n_seq * seq_len
        cap = capacity_of(tokens, top_k, n_exp)
        all_tok = n_slots * tokens
        x = x_in.reshape(all_tok, d_model)
        dy = dy_in.reshape(all_tok, d_model)
        q_dim, kv_dim = heads * head_dim, kv_heads * head_dim
        wt_q = jnp.transpose(w_query[ZERO], (1, 2, 0)).reshape(q_dim, d_model)
        wt_k = jnp.transpose(w_key[ZERO], (1, 2, 0)).reshape(kv_dim, d_model)
        wt_v = jnp.transpose(w_value[ZERO], (1, 2, 0)).reshape(kv_dim, d_model)
        wo = w_out[ZERO].reshape(q_dim, d_model)

        ids = jnp.transpose(expert_id[:, ZERO], (0, 3, 1, 2)).reshape(n_slots, top_k, tokens)
        gates = jnp.transpose(gate_vals[:, ZERO], (0, 3, 1, 2)).reshape(n_slots, top_k, tokens).astype(F32)
        table = jnp.stack([choice_keys(ids, n_exp), gates])
        route_ins = [table] + [exchange(table, mask) for mask in range(1, N_DEV)]
        chunk = n_slots // CHUNKS
        near = chunk * tokens
        index = lax.axis_index('ep')
        place = jnp.stack([index // 2, index % 2]).astype(jnp.int32)
        keys_all, gates_all, offs = route_tables(index[None].astype(jnp.int32), route_ins, local_e, n_slots // CHUNKS)
        dy_parts, taken = [], 0
        for part, count in enumerate(DY_PARTS):
            span = dy[taken * near:(taken + count) * near]
            if part == 0:
                gathered = gather_rows(span)
            else:
                gathered = lax.all_gather(span, 'ep', axis=0, tiled=False)
            dy_parts += [(gathered, at) for at in range(count)]
            taken += count

        position = jnp.arange(seq_len, dtype=F32)
        inv_freq = ROPE_BASE ** (-jnp.arange(head_dim // 2, dtype=F32) / (head_dim // 2))
        angle_t = position[:, None] * inv_freq[None, :]
        cos_t, sin_t = jnp.cos(angle_t), jnp.sin(angle_t)
        tables = (jnp.concatenate([cos_t] * 4, axis=1), jnp.concatenate([-sin_t, sin_t] * 2, axis=1))
        norms = (norm_attn, norm_ffn)
        attn_w = (wt_q, wt_k, wt_v, wo)
        groups, taken = [], 0
        for count in U_PARTS:
            groups.append(attn_forward(place, taken * near, count * near, x, norms, tables, attn_w, heads, kv_heads, seq_len, tokens))
            taken += count
        u_pairs, group_of, bases, keeps, gifts, taken = [], [], [], [], [], 0
        for group, count in zip(groups, U_PARTS):
            u, hidden, keep, gift = group[:4]
            pair = gather_rows(u)
            keeps.append(keep)
            gifts.append(exchange(gift, 1))
            base, d_shared = shared_expert(u, hidden, dy, taken, s_gate[ZERO], s_up[ZERO], s_down[ZERO])
            bases.append(base)
            u_pairs += [(pair, at) for at in range(count)]
            group_of += [((hidden, *group[4:7], d_shared), at) for at in range(count)]
            taken += count

        assert U_PARTS == DY_PARTS
        weights = (e_gate[ZERO], e_up[ZERO], e_down[ZERO])
        saved = None
        n_pairs = N_DEV // 2
        routed, d_routed = [], []
        for part in range(CHUNKS):
            u_pair, u_at = u_pairs[part]
            dy_all, dy_at = dy_parts[part]
            y_sum, du_sum, saved = expert_pass(place, offs[part, :, :n_pairs * chunk + 1], keys_all, gates_all, u_pair, u_at * chunk, dy_all, dy_at * chunk, weights, saved, cap, tokens, part, CHUNKS)
            d_routed.append(reduce_rows(du_sum))
            routed.append(lax.psum_scatter(y_sum, 'ep', scatter_dimension=0, tiled=False))
        y = (jnp.concatenate(bases, axis=0) + jnp.concatenate(routed, axis=0)).astype(BF16)
        pieces = []
        for experts in GRAD_PARTS:
            pieces = expert_grads(offs[:, :, n_pairs * chunk], saved, experts, pieces)
        g_e_gate, g_e_up, g_e_down = pieces

        done, twin, g_norms = [], [], 0.0
        for part in range(CHUNKS):
            *done, theirs, g_norm = attn_backward(place, part * near, near, x, dy, *group_of[part], d_routed[part],
                                                  norms, tables, attn_w, heads, kv_heads, seq_len, tokens, done)
            twin.append(exchange(theirs, 1))
            g_norms = g_norms + g_norm[ZERO]
        dx, d_hidden, mine = done
        g_norms = small_all_reduce(g_norms)
        dense_in = (keeps, gifts, mine, d_hidden, twin, 256)
        sent = dense_grads(place, False, *dense_in)
        kept = dense_grads(place, True, *dense_in)
        g_q, g_k, g_v, g_out = all_reduce_rows(place, kept, sent, (q_dim, kv_dim, kv_dim, q_dim))

        sums, taken = [], 0
        for count in U_PARTS:
            sums = shared_grads(place, u_pairs[taken][ZERO], dy_parts[taken][ZERO], near, count, s_gate[ZERO], s_up[ZERO], s_down[ZERO], sums)
            taken += count
        twins = [exchange(half, 1) for half in sums]
        side = s_gate.shape[2] // 2
        g_s_gate = join(sums[ZERO][:, :side], twins[ZERO][:, :side], index % 2, 1)
        g_s_up = join(sums[ZERO][:, side:], twins[ZERO][:, side:], index % 2, 1)
        g_s_down = join(sums[ONE], twins[ONE], index % 2, 0)
        g_norm_a, g_norm_f = g_norms[ZERO], g_norms[ONE]
        return (
            y.reshape(x_in.shape), dx.reshape(x_in.shape), g_norm_a[None],
            jnp.transpose(g_q.reshape(heads, head_dim, d_model), (2, 0, 1))[None],
            jnp.transpose(g_k.reshape(kv_heads, head_dim, d_model), (2, 0, 1))[None],
            jnp.transpose(g_v.reshape(kv_heads, head_dim, d_model), (2, 0, 1))[None],
            g_out.reshape(heads, head_dim, d_model)[None], g_norm_f[None], g_s_gate[None], g_s_up[None], g_s_down[None],
            g_e_gate[None], g_e_up[None], g_e_down[None],
        )

    tok_spec = P(None, ('dp', 'ep'), None, None)
    route_spec = P(None, None, ('dp', 'ep'), None, None)
    rep_spec = P()
    exp_spec = P(None, 'ep', None, None)
    vec_grad = P('dp', None)
    mat_grad = P('dp', None, None)
    head_grad = P('dp', None, None, None)
    exp_grad = P('dp', 'ep', None, None)
    in_specs = (tok_spec, tok_spec, route_spec, route_spec) + (rep_spec,) * 9 + (exp_spec,) * 3
    out_specs = (tok_spec, tok_spec, vec_grad, head_grad, head_grad, head_grad, head_grad, vec_grad, mat_grad, mat_grad, mat_grad, exp_grad, exp_grad, exp_grad)
    return jax.shard_map(device_body, mesh=mesh, in_specs=in_specs, out_specs=out_specs, check_vma=False)
```
